32 devices in a mesh: gx: 8 (over z, x), gy: 2 (over y), gz: 2 (over core).
Axes of the slice: x: 2, y: 2, z: 4, core: 2. Of those that a mesh axis runs over, the one named last changes fastest.
Arguments:
- velocity_term: float32 [32, 64, 256], P('gx', 'gy', 'gz'), may hold values from 0.05 to 0.2
- model_step: float32 [32, 64, 256], P('gx', 'gy', 'gz'), may hold values from -6 to 6
- background: bfloat16 [4, 32, 64, 256], P(None, 'gx', 'gy', 'gz'), may hold values from -6 to 6
- receivers: int32 [3, 256], replicated, may hold values from 0 to 255, as said below
- checkpoints: int32 [16], replicated, may hold values from 0 to 3, as said below
Outputs:
- image: float32 [32, 64, 256], P('gx', 'gy', 'gz')
- traces: float32 [16, 256], replicated
- column_image: float32 [32, 64], P('gx', 'gy')
- wavefield: float32 [32, 64, 256], P('gx', 'gy', 'gz')
The draws below stay inside these ranges and needn't reach their ends.
Inputs may be any that keep to these rules, and one draw needn't show every extreme that they name: receivers[0] indexes the first lateral dimension (below 32), receivers[1] the second (below 64), receivers[2] depth (below 256). `checkpoints`: never falling over the time steps, beginning at 0 and ending at 3.
All inputs are finite; a program needn't handle non-finite values.
Results may differ from the reference program's by a relative error of at most 0.0003.
Values sent between devices are 32-bit elements; how exact they have to be, the bound alone decides.
A program may use at most 64 MiB of HBM per device.

```python
import jax
import jax.numpy as jnp
from jax import lax

NT = 16
NCK = 4
RECV = 256
NX = 32
NY = 64
NZ = 256


def draw_receivers(key, part):
    key_x = jax.random.fold_in(key, 11)
    key_y = jax.random.fold_in(key, 12)
    key_z = jax.random.fold_in(key, 13)
    first = jax.random.randint(key_x, (RECV,), 0, NX)
    second = jax.random.randint(key_y, (RECV,), 0, NY)
    third = jax.random.randint(key_z, (RECV,), 0, NZ)
    return jnp.stack([first, second, third]).astype(jnp.int32)


def draw_checkpoints(key, part):
    inner = jax.random.fold_in(key, 21)
    values = jnp.sort(jax.random.randint(inner, (NT,), 0, NCK))
    values = values.at[0].set(0).at[NT - 1].set(NCK - 1)
    return values.astype(jnp.int32)


def block_levels(key, shape, pieces, smallest, top_value):
    gain, own = 1.0, jax.random.fold_in(key, 6)
    for dim, shards_of in pieces:
        steps = jnp.exp(jax.random.uniform(jax.random.fold_in(own, dim), (shards_of,), jnp.float32, smallest / len(pieces), top_value / len(pieces)))
        gain = gain * jnp.repeat(steps, shape[dim] // shards_of).reshape([-1 if axis == dim else 1 for axis in range(len(shape))])
    return gain


def centred(rng, dims, width, most, cuts=(), kind=jnp.bfloat16):
    array = width * jax.random.normal(rng, dims, jnp.float32)
    if cuts:
        array = array * block_levels(rng, dims, cuts, -0.22, 0.18)
    return jnp.clip(array, -most, most).astype(kind)


def setup_inputs(seed: int = 0) -> dict:
    seeds = jax.random.split(jax.random.key(seed), 6)
    return {
        "velocity_term": jnp.clip(0.05 + 0.15 * jax.random.uniform(seeds[0], (NX, NY, NZ), jnp.float32) ** block_levels(seeds[0], (NX, NY, NZ), ((0, 8), (1, 2), (2, 2)), -0.2, 0.2), 0.05, 0.2),
        "model_step": centred(seeds[1], (NX, NY, NZ), 1.0, 6.0, ((0, 8), (1, 2), (2, 2)), jnp.float32),
        "background": centred(seeds[2], (NCK, NX, NY, NZ), 1.0, 6.0, ((1, 8), (2, 2), (3, 2))),
        "receivers": draw_receivers(jax.random.fold_in(seeds[5], 71), 0),
        "checkpoints": draw_checkpoints(jax.random.fold_in(seeds[5], 71), 0),
    }


near_coef = 4.0 / 3.0
far_coef = -1.0 / 12.0
center_coef = -2.5


def laplace(field):
    total = 3.0 * center_coef * field
    for dim in (0, 1):
        total = total + near_coef * (jnp.roll(field, 1, dim) + jnp.roll(field, -1, dim))
        total = total + far_coef * (jnp.roll(field, 2, dim) + jnp.roll(field, -2, dim))
    padded = jnp.pad(field, ((0, 0), (0, 0), (2, 2)))
    total = total + near_coef * (padded[:, :, 3:-1] + padded[:, :, 1:-3])
    total = total + far_coef * (padded[:, :, 4:] + padded[:, :, :-4])
    return total


def reference(velocity_term, model_step, background, receivers, checkpoints):
    rec_x = receivers[0]
    rec_y = receivers[1]
    rec_z = receivers[2]
    zeros = jnp.zeros(model_step.shape, jnp.float32)
    previous = zeros
    current = zeros
    samples = []
    for step in range(NT):
        accel = lax.dynamic_index_in_dim(background, checkpoints[step], 0, keepdims=False).astype(jnp.float32)
        following = 2.0 * current - previous + velocity_term * laplace(current) + model_step * accel
        samples.append(following[rec_x, rec_y, rec_z])
        previous = current
        current = following
    traces = jnp.stack(samples)
    wavefield = current
    later_two = zeros
    later = zeros
    image = zeros
    for back in range(NT):
        step = NT - 1 - back
        accel = lax.dynamic_index_in_dim(background, checkpoints[step], 0, keepdims=False).astype(jnp.float32)
        adjoint = 2.0 * later - later_two + laplace(velocity_term * later)
        adjoint = adjoint.at[rec_x, rec_y, rec_z].add(traces[step])
        image = image + adjoint * accel
        later_two = later
        later = adjoint
    column_image = jnp.sum(image, axis=2) / NZ
    return image, traces, column_image, wavefield
```

```python
import functools

import jax
import jax.numpy as jnp
from jax import lax
from jax.experimental import pallas as pl
from jax.experimental.pallas import tpu as pltpu
from jax.sharding import PartitionSpec as P

near_coef = 4.0 / 3.0
far_coef = -1.0 / 12.0
center_coef = -2.5


def with_halo(block, sides, width, periodic):
    for axis, dim in sides:
        count = lax.axis_size(axis)
        forward = [(i, i + 1) for i in range(count - 1)]
        if periodic:
            forward.append((count - 1, 0))
        backward = [(target, source) for source, target in forward]
        low = lax.ppermute(
            lax.slice_in_dim(block, block.shape[dim] - width, None, axis=dim), axis, forward
        )
        high = lax.ppermute(lax.slice_in_dim(block, 0, width, axis=dim), axis, backward)
        block = jnp.concatenate([low, block, high], axis=dim)
    return block


def along(padded, dim):
    count = padded.shape[dim]
    first = lax.slice_in_dim(padded, 3, count - 1, axis=dim) + lax.slice_in_dim(
        padded, 1, count - 3, axis=dim
    )
    second = lax.slice_in_dim(padded, 4, count, axis=dim) + lax.slice_in_dim(
        padded, 0, count - 4, axis=dim
    )
    return near_coef * first + far_coef * second


def laplace(field):
    side = with_halo(field, (("gx", 0), ("gy", 1)), 2, True)
    deep = with_halo(field, (("gz", 2),), 2, False)
    x_pad = side[:, 2:-2, :]
    y_pad = side[2:-2, :, :]
    return 3.0 * center_coef * field + along(x_pad, 0) + along(y_pad, 1) + along(deep, 2)


def sample_row(samples, field, step, clip_x, clip_y, clip_z, inside):
    values = field[clip_x, clip_y, clip_z] * inside
    return lax.dynamic_update_index_in_dim(samples, values, step, 0)


def on_device(velocity_term, model_step, background, receivers, checkpoints):
    size_x, size_y, size_z = model_step.shape
    steps = checkpoints.shape[0]
    local_x = receivers[0] - lax.axis_index("gx") * size_x
    local_y = receivers[1] - lax.axis_index("gy") * size_y
    local_z = receivers[2] - lax.axis_index("gz") * size_z
    inside = (
        (local_x >= 0)
        & (local_x < size_x)
        & (local_y >= 0)
        & (local_y < size_y)
        & (local_z >= 0)
        & (local_z < size_z)
    )
    inside = inside.astype(jnp.float32)
    clip_x = jnp.clip(local_x, 0, size_x - 1)
    clip_y = jnp.clip(local_y, 0, size_y - 1)
    clip_z = jnp.clip(local_z, 0, size_z - 1)
    zeros = jnp.zeros(model_step.shape, jnp.float32)
    record = jnp.zeros((steps, receivers.shape[1]), jnp.float32)

    def forward(step, carry):
        previous, current, samples = carry
        accel = lax.dynamic_index_in_dim(background, checkpoints[step], 0, keepdims=False).astype(
            jnp.float32
        )
        following = 2.0 * current - previous + velocity_term * laplace(current) + model_step * accel
        samples = sample_row(samples, following, step, clip_x, clip_y, clip_z, inside)
        return (current, following, samples)

    previous, current, record = lax.fori_loop(0, steps, forward, (zeros, zeros, record))
    traces = lax.psum(record, ("gx", "gy", "gz"))

    def adjoint_step(back, carry):
        later_two, later, image = carry
        step = steps - 1 - back
        accel = lax.dynamic_index_in_dim(background, checkpoints[step], 0, keepdims=False).astype(
            jnp.float32
        )
        adjoint = 2.0 * later - later_two + laplace(velocity_term * later)
        inject = lax.dynamic_index_in_dim(traces, step, 0, keepdims=False) * inside
        adjoint = adjoint.at[clip_x, clip_y, clip_z].add(inject)
        return (later, adjoint, image + adjoint * accel)

    later_two, later, image = lax.fori_loop(0, steps, adjoint_step, (zeros, zeros, zeros))
    depth_total = size_z * lax.axis_size("gz")
    column_image = lax.psum(jnp.sum(image, axis=2), "gz") / depth_total
    return (image, traces, column_image, current)


MESH = pl.DeviceIdType.MESH
BLOCK = 4
GROUP = 4


def place_of(p, gxs, gys, gzs):
    q, gz = p // gzs, p % gzs
    per = 2 * gys
    zz, w = q // per, q % per
    w = w + (zz % 2) * (per - 1 - 2 * w)
    xx, yy = w // gys, w % gys
    return 2 * zz + xx, yy + xx * (gys - 1 - 2 * yy), gz


def position_of(gx, gy, gz, gxs, gys, gzs):
    per = 2 * gys
    zz, xx = gx // 2, gx % 2
    w = xx * gys + gy + xx * (gys - 1 - 2 * gy)
    w = w + (zz % 2) * (per - 1 - 2 * w)
    return (zz * per + w) * gzs + gz


def lateral(f, sx, sy, gys):
    rows, lanes = f.shape[1], f.shape[2]
    lane = lax.broadcasted_iota(jnp.int32, f.shape, 2)
    row = lax.broadcasted_iota(jnp.int32, f.shape, 1)
    yl = lane % sy

    def rr(a, k):
        return pltpu.roll(a, k % rows, 1) if k % rows else a

    def lr(a, k):
        return pltpu.roll(a, k % lanes, 2) if k % lanes else a

    gy = row % gys
    up = jnp.where(gy == gys - 1, rr(f, gys - 1), rr(f, -1))
    down = up if gys == 2 else jnp.where(gy == 0, rr(f, 1 - gys), rr(f, 1))
    fu, fd = lr(up, sy), lr(down, -sy)
    y1 = lr(jnp.where(yl >= 1, f, fu), -1) + lr(jnp.where(yl < sy - 1, f, fd), 1)
    y2 = lr(jnp.where(yl >= 2, f, fu), -2) + lr(jnp.where(yl < sy - 2, f, fd), 2)
    xu, xd = rr(f, -gys), rr(f, gys)
    x1 = lr(jnp.where(lane >= sy, f, xu), -sy) + lr(jnp.where(lane < lanes - sy, f, xd), sy)
    x2 = lr(jnp.where(lane >= 2 * sy, f, xu), -2 * sy) + lr(jnp.where(lane < lanes - 2 * sy, f, xd), 2 * sy)
    return near_coef * (x1 + y1) + far_coef * (x2 + y2)


def chain_kernel(
    dims, v_ref, m_ref, bg_ref, rec_ref, ck_ref,
    image_ref, traces_ref, column_ref, wave_ref,
    stage, landed, coef, own_bg, hist, adj, wbuf, img, count, fr, part, tr1, tr2, back_w, back_i, in_w, in_i,
    s_in, r_in, s_c, r_c, s_f, r_f, s_t, r_t, s_w, r_w, s_i, r_i,
):
    gxs, gys, gzs, sx, sy, sz, nck, steps = dims
    n = gxs * gys * gzs
    rows = gxs * gys
    lanes = sx * sy
    nz = sz * gzs // n
    per = sz // nz
    fields = 2 + nck
    gx, gy, gz = lax.axis_index("gx"), lax.axis_index("gy"), lax.axis_index("gz")
    pos = position_of(gx, gy, gz, gxs, gys, gzs)
    my_row = gx * gys + gy
    lo_id = place_of(jnp.maximum(pos - 1, 0), gxs, gys, gzs)
    hi_id = place_of(jnp.minimum(pos + 1, n - 1), gxs, gys, gzs)
    has_lo, has_hi = pos > 0, pos < n - 1
    ext = 3 * nz
    near_halo = 2 * (BLOCK - 1)

    def remote(src, dst, ss, rs, where):
        return pltpu.make_async_remote_copy(
            src_ref=src, dst_ref=dst, send_sem=ss, recv_sem=rs, device_id=where, device_id_type=MESH
        )

    fr[...] = jnp.zeros_like(fr)
    for f in range(1 + nck):
        coef[f, 0:nz] = jnp.zeros((nz, rows, lanes), jnp.float32)
        coef[f, 2 * nz :] = jnp.zeros((nz, rows, lanes), jnp.float32)

    barrier = pltpu.get_barrier_semaphore()

    def greet(p, carry):
        @pl.when(p != pos)
        def _():
            pl.semaphore_signal(barrier, inc=1, device_id=place_of(p, gxs, gys, gzs), device_id_type=MESH)
        return carry

    lax.fori_loop(0, n, greet, 0)

    for f in range(fields):
        if f == 0:
            block = v_ref[...]
        elif f == 1:
            block = m_ref[...]
        else:
            block = bg_ref[f - 2].astype(jnp.float32)
        turned = block.reshape(lanes, sz).T
        stage[:, f * nz : (f + 1) * nz, :] = turned.reshape(per, nz, lanes)
    pl.semaphore_wait(barrier, n - 1)

    slab = fields * nz

    def arrival(row):
        return landed.at[pl.ds(pl.multiple_of(row * slab, nz), slab)]

    def scatter_in(c, carry):
        p = gz * per + c

        @pl.when(p != pos)
        def _():
            remote(stage.at[c], arrival(my_row), s_in.at[c], r_in.at[my_row], place_of(p, gxs, gys, gzs)).start()

        @pl.when(p == pos)
        def _():
            landed[pl.ds(pl.multiple_of(my_row * slab, nz), slab), :] = stage[c]

        return carry

    lax.fori_loop(0, per, scatter_in, 0)

    rec = rec_ref[...]
    rx, ry, rz = rec[0:1], rec[1:2], rec[2:3]
    nrec = rec.shape[1]
    rrow = (rx // sx) * gys + ry // sy
    rlane = (rx % sx) * sy + ry % sy
    rlocal = rz - (pos - 1) * nz
    zr = jnp.where((rlocal >= 0) & (rlocal < ext), rlocal * rows + rrow, -1)
    one_zr = (lax.broadcasted_iota(jnp.int32, (ext * rows, nrec), 0) == zr).astype(jnp.float32)
    one_lane = (lax.broadcasted_iota(jnp.int32, (lanes, nrec), 0) == rlane).astype(jnp.float32)
    counted = lax.dot_general(
        one_zr.astype(jnp.bfloat16), one_lane.astype(jnp.bfloat16), (((1,), (1,)), ((), ())),
        preferred_element_type=jnp.float32,
    )
    count[...] = counted.reshape(ext, rows, lanes)
    hist[0] = jnp.zeros((ext, rows, lanes), jnp.float32)
    hist[1] = jnp.zeros((ext, rows, lanes), jnp.float32)
    adj[steps] = jnp.zeros((ext, rows, lanes), jnp.float32)
    adj[steps + 1] = jnp.zeros((ext, rows, lanes), jnp.float32)
    img[...] = jnp.zeros_like(img)

    owner = pos // per

    def wait_in(row, carry):
        sender = row // gys, row % gys, owner

        @pl.when((row != my_row) | (owner != gz))
        def _():
            remote(stage.at[0], arrival(row), s_in.at[0], r_in.at[row], sender).wait_recv()

        return carry

    lax.fori_loop(0, rows, wait_in, 0)

    def sent_in(c, carry):
        @pl.when(gz * per + c != pos)
        def _():
            remote(stage.at[c], arrival(my_row), s_in.at[c], r_in.at[my_row], lo_id).wait_send()

        return carry

    lax.fori_loop(0, per, sent_in, 0)

    for z in range(nz):
        def plane(f):
            return landed[pl.ds(f * nz + z, rows, stride=slab), :]

        coef[0, nz + z] = plane(0)
        model = plane(1)
        for k in range(nck):
            accel = plane(2 + k)
            own_bg[k, z] = accel
            coef[1 + k, nz + z] = model * accel

    def coef_copies():
        v_lo = remote(coef.at[0, pl.ds(nz, nz)], coef.at[0, pl.ds(2 * nz, nz)], s_c.at[0], r_c.at[0], lo_id)
        m_lo = remote(
            coef.at[pl.ds(1, nck), pl.ds(nz, near_halo)], coef.at[pl.ds(1, nck), pl.ds(2 * nz, near_halo)],
            s_c.at[1], r_c.at[1], lo_id,
        )
        v_hi = remote(coef.at[0, pl.ds(nz, nz)], coef.at[0, pl.ds(0, nz)], s_c.at[2], r_c.at[2], hi_id)
        m_hi = remote(
            coef.at[pl.ds(1, nck), pl.ds(2 * nz - near_halo, near_halo)],
            coef.at[pl.ds(1, nck), pl.ds(nz - near_halo, near_halo)],
            s_c.at[3], r_c.at[3], hi_id,
        )
        return (m_lo, v_lo), (m_hi, v_hi)

    def field_copies(e, newer, older):
        to_lo = [
            remote(a.at[pl.ds(nz, nz)], fr.at[e, 1, i], s_f.at[e, 0, i], r_f.at[e, 1, i], lo_id)
            for i, a in enumerate((newer, older))
        ]
        to_hi = [
            remote(a.at[pl.ds(nz, nz)], fr.at[e, 0, i], s_f.at[e, 1, i], r_f.at[e, 0, i], hi_id)
            for i, a in enumerate((newer, older))
        ]
        return to_lo, to_hi

    def launch(copies):
        to_lo, to_hi = copies

        @pl.when(has_hi)
        def _():
            for c in to_hi:
                c.start()

        @pl.when(has_lo)
        def _():
            for c in to_lo:
                c.start()

    def settle(copies):
        to_lo, to_hi = copies

        @pl.when(has_hi)
        def _():
            for c in to_lo:
                c.wait_recv()
            for c in to_hi:
                c.wait_send()

        @pl.when(has_lo)
        def _():
            for c in to_hi:
                c.wait_recv()
            for c in to_lo:
                c.wait_send()

    def fill(e, newer, older):
        for i, a in enumerate((newer, older)):
            a[0:nz] = fr[e, 0, i]
            a[2 * nz :] = fr[e, 1, i]

    def stencil(ref, at, size):
        f = ref[pl.ds(at, size)]
        first = ref[pl.ds(at + 1, size)] + ref[pl.ds(at - 1, size)]
        second = ref[pl.ds(at + 2, size)] + ref[pl.ds(at - 2, size)]
        return 3.0 * center_coef * f + lateral(f, sx, sy, gys) + near_coef * first + far_coef * second, f

    copies = coef_copies()
    launch(copies)
    settle(copies)

    def forward_block(b, carry):
        for j in range(BLOCK):
            step = b * BLOCK + j
            ck = ck_ref[step]
            lo = 2 * (j + 1)
            for at in range(lo, ext - lo, GROUP):
                size = min(GROUP, ext - lo - at)
                lap, f = stencil(hist.at[step + 1], at, size)
                src = coef[1 + ck, at : at + size]
                hist[step + 2, at : at + size] = (
                    2.0 * f - hist[step, at : at + size] + coef[0, at : at + size] * lap + src
                )
        newer, older = hist.at[(b + 1) * BLOCK + 1], hist.at[(b + 1) * BLOCK]
        moves = field_copies(b, newer, older)
        launch(moves)
        settle(moves)
        fill(b, newer, older)
        return carry

    blocks = steps // BLOCK
    lax.fori_loop(0, blocks, forward_block, 0)

    def send_back(src, dst, ss, rs, slot, g):
        def one(row, carry):
            other = (row != my_row) | (g != gz)

            @pl.when(other)
            def _():
                remote(src.at[row], dst.at[slot], ss.at[row], rs.at[slot], (row // gys, row % gys, g)).start()

            @pl.when(jnp.logical_not(other))
            def _():
                dst[slot] = src[row]

            return carry

        lax.fori_loop(0, rows, one, 0)

    def sent_back(src, dst, ss, rs, g):
        def one(row, carry):
            @pl.when((row != my_row) | (g != gz))
            def _():
                remote(src.at[row], dst.at[0], ss.at[row], rs.at[0], lo_id).wait_send()

            return carry

        lax.fori_loop(0, rows, one, 0)

    def got_back(src, dst, ss, rs, first, number):
        def one(c, carry):
            @pl.when(c + first != pos)
            def _():
                remote(src.at[0], dst.at[c], ss.at[0], rs.at[c], lo_id).wait_recv()

            return carry

        lax.fori_loop(0, number, one, 0)

    near = 4
    far = n // near
    team, seat = pos // near, pos % near

    def trace_sends(src, dst, kind):
        number = near if kind == 0 else far
        mine = seat if kind == 0 else team

        def one(i, carry):
            @pl.when(i != mine)
            def _():
                p = team * near + i if kind == 0 else i * near + seat
                remote(src, dst.at[mine], s_t.at[kind, i], r_t.at[kind, mine], place_of(p, gxs, gys, gzs)).start()

            return carry

        lax.fori_loop(0, number, one, 0)

    def trace_waits(src, dst, kind):
        number = near if kind == 0 else far
        mine = seat if kind == 0 else team

        def one(i, carry):
            @pl.when(i != mine)
            def _():
                remote(src, dst.at[i], s_t.at[kind, i], r_t.at[kind, i], lo_id).wait()

            return carry

        lax.fori_loop(0, number, one, 0)

    def gather_traces():
        picked = one_zr[nz * rows : 2 * nz * rows]
        lines = []
        for t in range(steps):
            table = hist[t + 2, nz : 2 * nz].reshape(nz * rows, lanes)
            at_lane = lax.dot_general(
                table, picked, (((0,), (0,)), ((), ())),
                preferred_element_type=jnp.float32, precision=lax.Precision.HIGHEST,
            )
            lines.append(jnp.sum(at_lane * one_lane, axis=0, keepdims=True))
        return jnp.concatenate(lines, axis=0)

    def adjoint_block(b, carry):
        for j in range(BLOCK):
            step = steps - 1 - b * BLOCK - j
            ck = ck_ref[step]
            lo = 2 * (j + 1)
            wbuf[lo - 2 : ext - lo + 2] = coef[0, lo - 2 : ext - lo + 2] * adj[step + 1, lo - 2 : ext - lo + 2]
            for at in range(lo, ext - lo, GROUP):
                size = min(GROUP, ext - lo - at)
                lap, f = stencil(wbuf, at, size)
                adj[step, at : at + size] = (
                    2.0 * adj[step + 1, at : at + size] - adj[step + 2, at : at + size] + lap
                    + count[at : at + size] * hist[step + 2, at : at + size]
                )
            img[...] += adj[step, nz : 2 * nz] * own_bg[ck]

        @pl.when(b < blocks - 1)
        def _():
            newer, older = adj.at[steps - (b + 1) * BLOCK], adj.at[steps - (b + 1) * BLOCK + 1]
            moves = field_copies(blocks + b, newer, older)
            launch(moves)

            @pl.when(b == 0)
            def _():
                part[0] = gather_traces()
                tr1[seat] = part[0]
                trace_sends(part.at[0], tr1, 0)
                for row in range(rows):
                    for z in range(nz):
                        back_w[row, z : z + 1] = hist[steps + 1, nz + z, row : row + 1]
                send_back(back_w, in_w, s_w, r_w, lax.rem(pos, per), owner)

            @pl.when(b == 1)
            def _():
                trace_waits(part.at[0], tr1, 0)
                total = tr1[0]
                for i in range(1, near):
                    total = total + tr1[i]
                part[1] = total
                tr2[team] = total
                trace_sends(part.at[1], tr2, 1)

            settle(moves)
            fill(blocks + b, newer, older)

        return carry

    lax.fori_loop(0, blocks, adjoint_block, 0)

    for row in range(rows):
        for z in range(nz):
            back_i[row, z : z + 1] = img[z, row : row + 1]
    for g in range(gzs):
        send_back(back_i, in_i, s_i.at[g], r_i, pos, g)

    trace_waits(part.at[1], tr2, 1)
    total = tr2[0]
    for i in range(1, far):
        total = total + tr2[i]
    traces_ref[...] = total
    got_back(back_w, in_w, s_w, r_w, gz * per, per)
    wave_ref[...] = in_w[...].reshape(sz, lanes).T.reshape(sx, sy, sz)
    sent_back(back_w, in_w, s_w, r_w, owner)

    got_back(back_i, in_i, s_i.at[0], r_i, 0, n)
    mine = in_i[pl.ds(gz * per, per)]
    image_ref[...] = mine.reshape(sz, lanes).T.reshape(sx, sy, sz)
    column_ref[...] = jnp.sum(in_i[...].reshape(n * nz, lanes), axis=0, keepdims=True) / (sz * gzs)
    for g in range(gzs):
        sent_back(back_i, in_i, s_i.at[g], r_i, g)


def chain_on_device(sizes, velocity_term, model_step, background, receivers, checkpoints):
    gxs, gys, gzs = sizes
    sx, sy, sz = model_step.shape
    nck, steps, nrec = background.shape[0], checkpoints.shape[0], receivers.shape[1]
    n, rows, lanes = gxs * gys * gzs, gxs * gys, sx * sy
    nz = sz * gzs // n
    per = sz // nz
    ext = 3 * nz
    blocks = steps // BLOCK
    dims = (gxs, gys, gzs, sx, sy, sz, nck, steps)
    f32 = jnp.float32
    dma = pltpu.SemaphoreType.DMA
    vmem = pl.BlockSpec(memory_space=pltpu.VMEM)
    image, traces, column, wave = pl.pallas_call(
        functools.partial(chain_kernel, dims),
        out_shape=(
            jax.ShapeDtypeStruct((sx, sy, sz), f32),
            jax.ShapeDtypeStruct((steps, nrec), f32),
            jax.ShapeDtypeStruct((1, lanes), f32),
            jax.ShapeDtypeStruct((sx, sy, sz), f32),
        ),
        in_specs=[vmem] * 4 + [pl.BlockSpec(memory_space=pltpu.SMEM)],
        out_specs=(vmem,) * 4,
        scratch_shapes=[
            pltpu.VMEM((per, (2 + nck) * nz, lanes), f32),
            pltpu.VMEM((rows * (2 + nck) * nz, lanes), f32),
            pltpu.VMEM((1 + nck, ext, rows, lanes), f32),
            pltpu.VMEM((nck, nz, rows, lanes), f32),
            pltpu.VMEM((steps + 2, ext, rows, lanes), f32),
            pltpu.VMEM((steps + 2, ext, rows, lanes), f32),
            pltpu.VMEM((ext, rows, lanes), f32),
            pltpu.VMEM((nz, rows, lanes), f32),
            pltpu.VMEM((ext, rows, lanes), f32),
            pltpu.VMEM((2 * blocks - 1, 2, 2, nz, rows, lanes), f32),
            pltpu.VMEM((2, steps, nrec), f32),
            pltpu.VMEM((4, steps, nrec), f32),
            pltpu.VMEM((n // 4, steps, nrec), f32),
            pltpu.VMEM((rows, nz, lanes), f32),
            pltpu.VMEM((rows, nz, lanes), f32),
            pltpu.VMEM((per, nz, lanes), f32),
            pltpu.VMEM((n, nz, lanes), f32),
            dma((per,)),
            dma((rows,)),
            dma((4,)),
            dma((4,)),
            dma((2 * blocks - 1, 2, 2)),
            dma((2 * blocks - 1, 2, 2)),
            dma((2, max(4, n // 4))),
            dma((2, max(4, n // 4))),
            dma((rows,)),
            dma((per,)),
            dma((gzs, rows)),
            dma((n,)),
        ],
        compiler_params=pltpu.CompilerParams(
            collective_id=0, has_side_effects=True, vmem_limit_bytes=48 * 1024 * 1024
        ),
    )(velocity_term, model_step, background, receivers, checkpoints)
    return image, traces, column.reshape(sx, sy), wave


def solution(mesh):
    gxs, gys, gzs = mesh.shape["gx"], mesh.shape["gy"], mesh.shape["gz"]
    n = gxs * gys * gzs

    def whole(velocity_term, model_step, background, receivers, checkpoints):
        nx, ny, depth = model_step.shape
        fits = (
            depth % (8 * n) == 0
            and depth // n == 2 * BLOCK
            and gxs % 2 == 0
            and (gxs * gys) % 8 == 0
            and n % 4 == 0
            and (nx // gxs) * (ny // gys) % 128 == 0
            and (ny // gys) % 8 == 0
            and nx // gxs >= 4
            and checkpoints.shape[0] % BLOCK == 0
        )
        body = functools.partial(chain_on_device, (gxs, gys, gzs)) if fits else on_device
        return jax.shard_map(
            body,
            mesh=mesh,
            in_specs=(P("gx", "gy", "gz"), P("gx", "gy", "gz"), P(None, "gx", "gy", "gz"), P(), P()),
            out_specs=(P("gx", "gy", "gz"), P(), P("gx", "gy"), P("gx", "gy", "gz")),
            check_vma=False,
        )(velocity_term, model_step, background, receivers, checkpoints)

    return whole
```

```python
import functools

import jax
import jax.numpy as jnp
from jax import lax
from jax.experimental import pallas as pl
from jax.experimental.pallas import tpu as pltpu
from jax.sharding import PartitionSpec as P

near_coef = 4.0 / 3.0
far_coef = -1.0 / 12.0
center_coef = -2.5


def with_halo(block, sides, width, periodic):
    for axis, dim in sides:
        count = lax.axis_size(axis)
        forward = [(i, i + 1) for i in range(count - 1)]
        if periodic:
            forward.append((count - 1, 0))
        backward = [(target, source) for source, target in forward]
        low = lax.ppermute(
            lax.slice_in_dim(block, block.shape[dim] - width, None, axis=dim), axis, forward
        )
        high = lax.ppermute(lax.slice_in_dim(block, 0, width, axis=dim), axis, backward)
        block = jnp.concatenate([low, block, high], axis=dim)
    return block


def along(padded, dim):
    count = padded.shape[dim]
    first = lax.slice_in_dim(padded, 3, count - 1, axis=dim) + lax.slice_in_dim(
        padded, 1, count - 3, axis=dim
    )
    second = lax.slice_in_dim(padded, 4, count, axis=dim) + lax.slice_in_dim(
        padded, 0, count - 4, axis=dim
    )
    return near_coef * first + far_coef * second


def laplace(field):
    side = with_halo(field, (("gx", 0), ("gy", 1)), 2, True)
    deep = with_halo(field, (("gz", 2),), 2, False)
    x_pad = side[:, 2:-2, :]
    y_pad = side[2:-2, :, :]
    return 3.0 * center_coef * field + along(x_pad, 0) + along(y_pad, 1) + along(deep, 2)


def sample_row(samples, field, step, clip_x, clip_y, clip_z, inside):
    values = field[clip_x, clip_y, clip_z] * inside
    return lax.dynamic_update_index_in_dim(samples, values, step, 0)


def on_device(velocity_term, model_step, background, receivers, checkpoints):
    size_x, size_y, size_z = model_step.shape
    steps = checkpoints.shape[0]
    local_x = receivers[0] - lax.axis_index("gx") * size_x
    local_y = receivers[1] - lax.axis_index("gy") * size_y
    local_z = receivers[2] - lax.axis_index("gz") * size_z
    inside = (
        (local_x >= 0)
        & (local_x < size_x)
        & (local_y >= 0)
        & (local_y < size_y)
        & (local_z >= 0)
        & (local_z < size_z)
    )
    inside = inside.astype(jnp.float32)
    clip_x = jnp.clip(local_x, 0, size_x - 1)
    clip_y = jnp.clip(local_y, 0, size_y - 1)
    clip_z = jnp.clip(local_z, 0, size_z - 1)
    zeros = jnp.zeros(model_step.shape, jnp.float32)
    record = jnp.zeros((steps, receivers.shape[1]), jnp.float32)

    def forward(step, carry):
        previous, current, samples = carry
        accel = lax.dynamic_index_in_dim(background, checkpoints[step], 0, keepdims=False).astype(
            jnp.float32
        )
        following = 2.0 * current - previous + velocity_term * laplace(current) + model_step * accel
        samples = sample_row(samples, following, step, clip_x, clip_y, clip_z, inside)
        return (current, following, samples)

    previous, current, record = lax.fori_loop(0, steps, forward, (zeros, zeros, record))
    traces = lax.psum(record, ("gx", "gy", "gz"))

    def adjoint_step(back, carry):
        later_two, later, image = carry
        step = steps - 1 - back
        accel = lax.dynamic_index_in_dim(background, checkpoints[step], 0, keepdims=False).astype(
            jnp.float32
        )
        adjoint = 2.0 * later - later_two + laplace(velocity_term * later)
        inject = lax.dynamic_index_in_dim(traces, step, 0, keepdims=False) * inside
        adjoint = adjoint.at[clip_x, clip_y, clip_z].add(inject)
        return (later, adjoint, image + adjoint * accel)

    later_two, later, image = lax.fori_loop(0, steps, adjoint_step, (zeros, zeros, zeros))
    depth_total = size_z * lax.axis_size("gz")
    column_image = lax.psum(jnp.sum(image, axis=2), "gz") / depth_total
    return (image, traces, column_image, current)


MESH = pl.DeviceIdType.MESH
BLOCK = 4
GROUP = 1


def place_of(p, gxs, gys, gzs):
    q, gz = p // gzs, p % gzs
    per = 2 * gys
    zz, w = q // per, q % per
    w = w + (zz % 2) * (per - 1 - 2 * w)
    xx, yy = w // gys, w % gys
    return 2 * zz + xx, yy + xx * (gys - 1 - 2 * yy), gz


def position_of(gx, gy, gz, gxs, gys, gzs):
    per = 2 * gys
    zz, xx = gx // 2, gx % 2
    w = xx * gys + gy + xx * (gys - 1 - 2 * gy)
    w = w + (zz % 2) * (per - 1 - 2 * w)
    return (zz * per + w) * gzs + gz


def lateral(f, sx, sy, gys):
    rows, lanes = f.shape[1], f.shape[2]
    lane = lax.broadcasted_iota(jnp.int32, f.shape, 2)
    row = lax.broadcasted_iota(jnp.int32, f.shape, 1)
    yl = lane % sy

    def rr(a, k):
        return pltpu.roll(a, k % rows, 1) if k % rows else a

    def lr(a, k):
        return pltpu.roll(a, k % lanes, 2) if k % lanes else a

    gy = row % gys
    up = jnp.where(gy == gys - 1, rr(f, gys - 1), rr(f, -1))
    down = up if gys == 2 else jnp.where(gy == 0, rr(f, 1 - gys), rr(f, 1))
    fu, fd = lr(up, sy), lr(down, -sy)
    y1 = lr(jnp.where(yl >= 1, f, fu), -1) + lr(jnp.where(yl < sy - 1, f, fd), 1)
    y2 = lr(jnp.where(yl >= 2, f, fu), -2) + lr(jnp.where(yl < sy - 2, f, fd), 2)
    xu, xd = rr(f, -gys), rr(f, gys)
    x1 = lr(jnp.where(lane >= sy, f, xu), -sy) + lr(jnp.where(lane < lanes - sy, f, xd), sy)
    x2 = lr(jnp.where(lane >= 2 * sy, f, xu), -2 * sy) + lr(jnp.where(lane < lanes - 2 * sy, f, xd), 2 * sy)
    return near_coef * (x1 + y1) + far_coef * (x2 + y2)


def chain_kernel(
    dims, v_hbm, m_hbm, bg_hbm, rec_hbm, ck_hbm,
    image_ref, traces_ref, column_ref, wave_ref,
    stage, landed, coef, own_bg, hist, adj, wbuf, img, count, fr, part, tr1, tr2, back_w, back_i, in_w, in_i,
    v_ref, m_ref, bg_ref, rec_ref, ck_ref, s_a, s_in, r_in, s_c, r_c, s_f, r_f, s_t, r_t, s_w, r_w, s_i, r_i,
):
    gxs, gys, gzs, sx, sy, sz, nck, steps = dims
    n = gxs * gys * gzs
    rows = gxs * gys
    lanes = sx * sy
    nz = sz * gzs // n
    per = sz // nz
    fields = 2 + nck
    gx, gy, gz = lax.axis_index("gx"), lax.axis_index("gy"), lax.axis_index("gz")
    pos = position_of(gx, gy, gz, gxs, gys, gzs)
    my_row = gx * gys + gy
    lo_id = place_of(jnp.maximum(pos - 1, 0), gxs, gys, gzs)
    hi_id = place_of(jnp.minimum(pos + 1, n - 1), gxs, gys, gzs)
    has_lo, has_hi = pos > 0, pos < n - 1
    ext = 3 * nz
    near_halo = 2 * (BLOCK - 1)

    def remote(src, dst, ss, rs, where):
        return pltpu.make_async_remote_copy(
            src_ref=src, dst_ref=dst, send_sem=ss, recv_sem=rs, device_id=where, device_id_type=MESH
        )

    fetches = [
        pltpu.make_async_copy(src, dst, s_a.at[i])
        for i, (src, dst) in enumerate(
            ((v_hbm, v_ref), (m_hbm, m_ref), (bg_hbm, bg_ref), (rec_hbm, rec_ref), (ck_hbm, ck_ref))
        )
    ]
    for fetch in fetches:
        fetch.start()

    fr[...] = jnp.zeros_like(fr)
    for f in range(1 + nck):
        coef[f, 0:nz] = jnp.zeros((nz, rows, lanes), jnp.float32)
        coef[f, 2 * nz :] = jnp.zeros((nz, rows, lanes), jnp.float32)

    barrier = pltpu.get_barrier_semaphore()

    def greet(p, carry):
        @pl.when(p != pos)
        def _():
            pl.semaphore_signal(barrier, inc=1, device_id=place_of(p, gxs, gys, gzs), device_id_type=MESH)
        return carry

    lax.fori_loop(0, n, greet, 0)

    for fetch in fetches:
        fetch.wait()
    for f in range(fields):
        if f == 0:
            block = v_ref[...]
        elif f == 1:
            block = m_ref[...]
        else:
            block = bg_ref[f - 2].astype(jnp.float32)
        turned = block.reshape(lanes, sz).T
        stage[:, f * nz : (f + 1) * nz, :] = turned.reshape(per, nz, lanes)
    pl.semaphore_wait(barrier, n - 1)

    slab = fields * nz

    def arrival(row):
        return landed.at[pl.ds(pl.multiple_of(row * slab, nz), slab)]

    def scatter_in(c, carry):
        p = gz * per + c

        @pl.when(p != pos)
        def _():
            remote(stage.at[c], arrival(my_row), s_in.at[c], r_in.at[my_row], place_of(p, gxs, gys, gzs)).start()

        @pl.when(p == pos)
        def _():
            landed[pl.ds(pl.multiple_of(my_row * slab, nz), slab), :] = stage[c]

        return carry

    lax.fori_loop(0, per, scatter_in, 0)

    rec = rec_ref[...]
    rx, ry, rz = rec[0:1], rec[1:2], rec[2:3]
    nrec = rec.shape[1]
    rrow = (rx // sx) * gys + ry // sy
    rlane = (rx % sx) * sy + ry % sy
    rlocal = rz - (pos - 1) * nz
    zr = jnp.where((rlocal >= 0) & (rlocal < ext), rlocal * rows + rrow, -1)
    one_zr = (lax.broadcasted_iota(jnp.int32, (ext * rows, nrec), 0) == zr).astype(jnp.float32)
    one_lane = (lax.broadcasted_iota(jnp.int32, (lanes, nrec), 0) == rlane).astype(jnp.float32)
    counted = lax.dot_general(
        one_zr.astype(jnp.bfloat16), one_lane.astype(jnp.bfloat16), (((1,), (1,)), ((), ())),
        preferred_element_type=jnp.float32,
    )
    count[...] = counted.reshape(ext, rows, lanes)
    hist[0] = jnp.zeros((ext, rows, lanes), jnp.float32)
    hist[1] = jnp.zeros((ext, rows, lanes), jnp.float32)
    adj[steps] = jnp.zeros((ext, rows, lanes), jnp.float32)
    adj[steps + 1] = jnp.zeros((ext, rows, lanes), jnp.float32)
    img[...] = jnp.zeros_like(img)

    owner = pos // per

    def wait_in(row, carry):
        sender = row // gys, row % gys, owner

        @pl.when((row != my_row) | (owner != gz))
        def _():
            remote(stage.at[0], arrival(row), s_in.at[0], r_in.at[row], sender).wait_recv()

        return carry

    lax.fori_loop(0, rows, wait_in, 0)

    def sent_in(c, carry):
        @pl.when(gz * per + c != pos)
        def _():
            remote(stage.at[c], arrival(my_row), s_in.at[c], r_in.at[my_row], lo_id).wait_send()

        return carry

    lax.fori_loop(0, per, sent_in, 0)

    for z in range(nz):
        def plane(f):
            return landed[pl.ds(f * nz + z, rows, stride=slab), :]

        coef[0, nz + z] = plane(0)
        model = plane(1)
        for k in range(nck):
            accel = plane(2 + k)
            own_bg[k, z] = accel
            coef[1 + k, nz + z] = model * accel

    def coef_copies():
        v_lo = remote(coef.at[0, pl.ds(nz, nz)], coef.at[0, pl.ds(2 * nz, nz)], s_c.at[0], r_c.at[0], lo_id)
        m_lo = remote(
            coef.at[pl.ds(1, nck), pl.ds(nz, near_halo)], coef.at[pl.ds(1, nck), pl.ds(2 * nz, near_halo)],
            s_c.at[1], r_c.at[1], lo_id,
        )
        v_hi = remote(coef.at[0, pl.ds(nz, nz)], coef.at[0, pl.ds(0, nz)], s_c.at[2], r_c.at[2], hi_id)
        m_hi = remote(
            coef.at[pl.ds(1, nck), pl.ds(2 * nz - near_halo, near_halo)],
            coef.at[pl.ds(1, nck), pl.ds(nz - near_halo, near_halo)],
            s_c.at[3], r_c.at[3], hi_id,
        )
        return (m_lo, v_lo), (m_hi, v_hi)

    def field_copies(e, field, older):
        i = 1 if older else 0
        near = near_halo if older else nz
        to_lo = remote(
            field.at[pl.ds(nz, near)], fr.at[e, 1, i, pl.ds(0, near)], s_f.at[e, 0, i], r_f.at[e, 1, i], lo_id
        )
        to_hi = remote(
            field.at[pl.ds(2 * nz - near, near)], fr.at[e, 0, i, pl.ds(nz - near, near)],
            s_f.at[e, 1, i], r_f.at[e, 0, i], hi_id,
        )
        return (to_lo,), (to_hi,)

    def launch(copies):
        to_lo, to_hi = copies

        @pl.when(has_hi)
        def _():
            for c in to_hi:
                c.start()

        @pl.when(has_lo)
        def _():
            for c in to_lo:
                c.start()

    def settle(copies):
        to_lo, to_hi = copies

        @pl.when(has_hi)
        def _():
            for c in to_lo:
                c.wait_recv()
            for c in to_hi:
                c.wait_send()

        @pl.when(has_lo)
        def _():
            for c in to_hi:
                c.wait_recv()
            for c in to_lo:
                c.wait_send()

    def fill(e, newer, older):
        for i, a in enumerate((newer, older)):
            near = near_halo if i else nz
            a[nz - near : nz] = fr[e, 0, i, nz - near :]
            a[2 * nz : 2 * nz + near] = fr[e, 1, i, :near]

    def stencil(ref, at, size):
        f = ref[pl.ds(at, size)]
        first = ref[pl.ds(at + 1, size)] + ref[pl.ds(at - 1, size)]
        second = ref[pl.ds(at + 2, size)] + ref[pl.ds(at - 2, size)]
        return 3.0 * center_coef * f + lateral(f, sx, sy, gys) + near_coef * first + far_coef * second, f

    copies = coef_copies()
    launch(copies)
    settle(copies)

    def forward_block(b, carry):
        newer, older = hist.at[(b + 1) * BLOCK + 1], hist.at[(b + 1) * BLOCK]
        for j in range(BLOCK):
            step = b * BLOCK + j
            ck = ck_ref[step]
            lo = 2 * (j + 1)
            for at in range(lo, ext - lo, GROUP):
                size = min(GROUP, ext - lo - at)
                lap, f = stencil(hist.at[step + 1], at, size)
                src = coef[1 + ck, at : at + size]
                hist[step + 2, at : at + size] = (
                    2.0 * f - hist[step, at : at + size] + coef[0, at : at + size] * lap + src
                )
            if j == BLOCK - 2:
                launch(field_copies(b, older, True))
        launch(field_copies(b, newer, False))
        settle(field_copies(b, older, True))
        settle(field_copies(b, newer, False))
        fill(b, newer, older)
        return carry

    blocks = steps // BLOCK
    lax.fori_loop(0, blocks, forward_block, 0)

    def send_back(src, dst, ss, rs, slot, g):
        def one(row, carry):
            other = (row != my_row) | (g != gz)

            @pl.when(other)
            def _():
                remote(src.at[row], dst.at[slot], ss.at[row], rs.at[slot], (row // gys, row % gys, g)).start()

            @pl.when(jnp.logical_not(other))
            def _():
                dst[slot] = src[row]

            return carry

        lax.fori_loop(0, rows, one, 0)

    def sent_back(src, dst, ss, rs, g):
        def one(row, carry):
            @pl.when((row != my_row) | (g != gz))
            def _():
                remote(src.at[row], dst.at[0], ss.at[row], rs.at[0], lo_id).wait_send()

            return carry

        lax.fori_loop(0, rows, one, 0)

    def got_back(src, dst, ss, rs, first, number):
        def one(c, carry):
            @pl.when(c + first != pos)
            def _():
                remote(src.at[0], dst.at[c], ss.at[0], rs.at[c], lo_id).wait_recv()

            return carry

        lax.fori_loop(0, number, one, 0)

    near = 4
    far = n // near
    team, seat = pos // near, pos % near

    def trace_sends(src, dst, kind):
        number = near if kind == 0 else far
        mine = seat if kind == 0 else team

        def one(i, carry):
            @pl.when(i != mine)
            def _():
                p = team * near + i if kind == 0 else i * near + seat
                remote(src, dst.at[mine], s_t.at[kind, i], r_t.at[kind, mine], place_of(p, gxs, gys, gzs)).start()

            return carry

        lax.fori_loop(0, number, one, 0)

    def trace_waits(src, dst, kind):
        number = near if kind == 0 else far
        mine = seat if kind == 0 else team

        def one(i, carry):
            @pl.when(i != mine)
            def _():
                remote(src, dst.at[i], s_t.at[kind, i], r_t.at[kind, i], lo_id).wait()

            return carry

        lax.fori_loop(0, number, one, 0)

    def gather_traces():
        picked = one_zr[nz * rows : 2 * nz * rows]
        lines = []
        for t in range(steps):
            table = hist[t + 2, nz : 2 * nz].reshape(nz * rows, lanes)
            at_lane = lax.dot_general(
                table, picked, (((0,), (0,)), ((), ())),
                preferred_element_type=jnp.float32, precision=lax.Precision.HIGHEST,
            )
            lines.append(jnp.sum(at_lane * one_lane, axis=0, keepdims=True))
        return jnp.concatenate(lines, axis=0)

    def adjoint_block(b, carry):
        newer, older = adj.at[steps - (b + 1) * BLOCK], adj.at[steps - (b + 1) * BLOCK + 1]
        for j in range(BLOCK):
            step = steps - 1 - b * BLOCK - j
            ck = ck_ref[step]
            lo = 2 * (j + 1)
            wbuf[lo - 2 : ext - lo + 2] = coef[0, lo - 2 : ext - lo + 2] * adj[step + 1, lo - 2 : ext - lo + 2]
            for at in range(lo, ext - lo, GROUP):
                size = min(GROUP, ext - lo - at)
                lap, f = stencil(wbuf, at, size)
                adj[step, at : at + size] = (
                    2.0 * adj[step + 1, at : at + size] - adj[step + 2, at : at + size] + lap
                    + count[at : at + size] * hist[step + 2, at : at + size]
                )
            if j == BLOCK - 2:

                @pl.when(b < blocks - 1)
                def _():
                    launch(field_copies(blocks + b, older, True))

            if j < BLOCK - 1:
                img[...] += adj[step, nz : 2 * nz] * own_bg[ck]

        @pl.when(b < blocks - 1)
        def _():
            launch(field_copies(blocks + b, newer, False))

        img[...] += adj[step, nz : 2 * nz] * own_bg[ck]

        @pl.when(b < blocks - 1)
        def _():

            @pl.when(b == 0)
            def _():
                part[0] = gather_traces()
                tr1[seat] = part[0]
                trace_sends(part.at[0], tr1, 0)
                for row in range(rows):
                    for z in range(nz):
                        back_w[row, z : z + 1] = hist[steps + 1, nz + z, row : row + 1]
                send_back(back_w, in_w, s_w, r_w, lax.rem(pos, per), owner)

            @pl.when(b == 1)
            def _():
                trace_waits(part.at[0], tr1, 0)
                total = tr1[0]
                for i in range(1, near):
                    total = total + tr1[i]
                part[1] = total
                tr2[team] = total
                trace_sends(part.at[1], tr2, 1)

            settle(field_copies(blocks + b, older, True))
            settle(field_copies(blocks + b, newer, False))
            fill(blocks + b, newer, older)

        return carry

    lax.fori_loop(0, blocks, adjoint_block, 0)

    for row in range(rows):
        for z in range(nz):
            back_i[row, z : z + 1] = img[z, row : row + 1]
    for g in range(gzs):
        send_back(back_i, in_i, s_i.at[g], r_i, pos, g)

    trace_waits(part.at[1], tr2, 1)
    total = tr2[0]
    for i in range(1, far):
        total = total + tr2[i]
    traces_ref[...] = total
    got_back(back_w, in_w, s_w, r_w, gz * per, per)
    wave_ref[...] = in_w[...].reshape(sz, lanes).T.reshape(sx, sy, sz)
    sent_back(back_w, in_w, s_w, r_w, owner)

    got_back(back_i, in_i, s_i.at[0], r_i, 0, n)
    mine = in_i[pl.ds(gz * per, per)]
    image_ref[...] = mine.reshape(sz, lanes).T.reshape(sx, sy, sz)
    column = jnp.sum(in_i[...].reshape(n * nz, lanes), axis=0, keepdims=True) / (sz * gzs)
    for x in range(sx):
        column_ref[x : x + 1, :] = column[:, x * sy : (x + 1) * sy]
    for g in range(gzs):
        sent_back(back_i, in_i, s_i.at[g], r_i, g)


def write_out(*refs):
    copies = [pltpu.make_async_copy(refs[i], refs[4 + i], refs[8].at[i]) for i in range(4)]
    for copy in copies:
        copy.start()
    for copy in copies:
        copy.wait()


def chain_on_device(sizes, velocity_term, model_step, background, receivers, checkpoints):
    gxs, gys, gzs = sizes
    sx, sy, sz = model_step.shape
    nck, steps, nrec = background.shape[0], checkpoints.shape[0], receivers.shape[1]
    n, rows, lanes = gxs * gys * gzs, gxs * gys, sx * sy
    nz = sz * gzs // n
    per = sz // nz
    ext = 3 * nz
    blocks = steps // BLOCK
    dims = (gxs, gys, gzs, sx, sy, sz, nck, steps)
    f32 = jnp.float32
    dma = pltpu.SemaphoreType.DMA
    vmem = pl.BlockSpec(memory_space=pltpu.VMEM)
    hbm = pl.BlockSpec(memory_space=pltpu.HBM)
    results = pl.pallas_call(
        functools.partial(chain_kernel, dims),
        out_shape=(
            jax.ShapeDtypeStruct((sx, sy, sz), f32),
            jax.ShapeDtypeStruct((steps, nrec), f32),
            jax.ShapeDtypeStruct((sx, sy), f32),
            jax.ShapeDtypeStruct((sx, sy, sz), f32),
        ),
        in_specs=[hbm] * 5,
        out_specs=(vmem,) * 4,
        scratch_shapes=[
            pltpu.VMEM((per, (2 + nck) * nz, lanes), f32),
            pltpu.VMEM((rows * (2 + nck) * nz, lanes), f32),
            pltpu.VMEM((1 + nck, ext, rows, lanes), f32),
            pltpu.VMEM((nck, nz, rows, lanes), f32),
            pltpu.VMEM((steps + 2, ext, rows, lanes), f32),
            pltpu.VMEM((steps + 2, ext, rows, lanes), f32),
            pltpu.VMEM((ext, rows, lanes), f32),
            pltpu.VMEM((nz, rows, lanes), f32),
            pltpu.VMEM((ext, rows, lanes), f32),
            pltpu.VMEM((2 * blocks - 1, 2, 2, nz, rows, lanes), f32),
            pltpu.VMEM((2, steps, nrec), f32),
            pltpu.VMEM((4, steps, nrec), f32),
            pltpu.VMEM((n // 4, steps, nrec), f32),
            pltpu.VMEM((rows, nz, lanes), f32),
            pltpu.VMEM((rows, nz, lanes), f32),
            pltpu.VMEM((per, nz, lanes), f32),
            pltpu.VMEM((n, nz, lanes), f32),
            pltpu.VMEM(velocity_term.shape, f32),
            pltpu.VMEM(model_step.shape, f32),
            pltpu.VMEM(background.shape, background.dtype),
            pltpu.VMEM(receivers.shape, receivers.dtype),
            pltpu.SMEM(checkpoints.shape, checkpoints.dtype),
            dma((5,)),
            dma((per,)),
            dma((rows,)),
            dma((4,)),
            dma((4,)),
            dma((2 * blocks - 1, 2, 2)),
            dma((2 * blocks - 1, 2, 2)),
            dma((2, max(4, n // 4))),
            dma((2, max(4, n // 4))),
            dma((rows,)),
            dma((per,)),
            dma((gzs, rows)),
            dma((n,)),
        ],
        compiler_params=pltpu.CompilerParams(
            collective_id=0, has_side_effects=True, vmem_limit_bytes=67043328
        ),
    )(velocity_term, model_step, background, receivers, checkpoints)
    return tuple(
        pl.pallas_call(
            write_out,
            out_shape=tuple(jax.ShapeDtypeStruct(a.shape, a.dtype) for a in results),
            in_specs=[vmem] * 4,
            out_specs=(hbm,) * 4,
            scratch_shapes=[dma((4,))],
            compiler_params=pltpu.CompilerParams(vmem_limit_bytes=1024 * 1024),
        )(*results)
    )


def solution(mesh):
    gxs, gys, gzs = mesh.shape["gx"], mesh.shape["gy"], mesh.shape["gz"]
    n = gxs * gys * gzs

    def whole(velocity_term, model_step, background, receivers, checkpoints):
        nx, ny, depth = model_step.shape
        fits = (
            depth % (8 * n) == 0
            and depth // n == 2 * BLOCK
            and gxs % 2 == 0
            and (gxs * gys) % 8 == 0
            and n % 4 == 0
            and (nx // gxs) * (ny // gys) % 128 == 0
            and (ny // gys) % 8 == 0
            and nx // gxs >= 4
            and checkpoints.shape[0] % BLOCK == 0
        )
        body = functools.partial(chain_on_device, (gxs, gys, gzs)) if fits else on_device
        return jax.shard_map(
            body,
            mesh=mesh,
            in_specs=(P("gx", "gy", "gz"), P("gx", "gy", "gz"), P(None, "gx", "gy", "gz"), P(), P()),
            out_specs=(P("gx", "gy", "gz"), P(), P("gx", "gy"), P("gx", "gy", "gz")),
            check_vma=False,
        )(velocity_term, model_step, background, receivers, checkpoints)

    return whole
```
